256 devices in a mesh: exp: 32 (over x, y, core), tp: 8 (over z).
Axes of the slice: x: 4, y: 4, z: 8, core: 2. Of those that a mesh axis runs over, the one named last changes fastest.
Arguments:
- tokens: bfloat16 [896, 4096], P('exp', 'tp'), may hold values from -6 to 6
- cotangent: bfloat16 [896, 4096], P('exp', 'tp'), may hold values from -6 to 6
- experts: int32 [896, 2], P('exp'), may hold values from 0 to 7, all different within a row; in each aligned block of 28 rows (0 to 27, 28 to 55, ...) at most 8 rows name the same one
- gates: float32 [896, 2], P('exp'), may hold values from 0.1 to 0.9
- w_gate: bfloat16 [32, 4096, 2048], P('exp', None, 'tp'), may hold values from -0.09375 to 0.09375
- w_up: bfloat16 [32, 4096, 2048], P('exp', None, 'tp'), may hold values from -0.09375 to 0.09375
- w_down: bfloat16 [32, 2048, 4096], P('exp', 'tp'), may hold values from -0.0625 to 0.0625
Outputs:
- output: bfloat16 [896, 4096], P('exp', 'tp')
- input_grad: bfloat16 [896, 4096], P('exp', 'tp')
- grad_gate: bfloat16 [32, 4096, 2048], P('exp', None, 'tp')
- grad_up: bfloat16 [32, 4096, 2048], P('exp', None, 'tp')
- grad_down: bfloat16 [32, 2048, 4096], P('exp', 'tp')
The draws below stay inside these ranges and needn't reach their ends.
Inputs may be any that keep to these rules, and one draw needn't show every extreme that they name: Each row names 2 different experts. In each aligned block of 28 rows (the rows of one index of exp) no expert is named by more than 8 rows, and in some blocks one is named by exactly 8.
All inputs are finite; a program needn't handle non-finite values.
Results may differ from the reference program's by a relative error of at most 0.017.
Values may be sent and summed in bfloat16 or wider, within the bound.
No kernel may reach another device: no remote copies, remote signals or barrier semaphores. Data moves between devices by JAX's collectives and lax.ppermute only.
A program may use at most 64 MiB of HBM per device.

```python
import math
import jax
import jax.numpy as jnp
import numpy as np
from jax import lax

D = 4096
FF = 8192
EXPERTS = 8
TOP = 2
TOK_DEV = 28
CAP = 8
GROUP = 4
TOKENS = 896
N_EXP = 32


def shard_levels(rng, shape, split, low, largest):
    gain = 1.0
    for dim, shards_of in split:
        draws = jax.random.uniform(jax.random.fold_in(jax.random.fold_in(rng, 6), dim), (shards_of,), jnp.float32, low / len(split), largest / len(split))
        gain = gain * jnp.repeat(jnp.exp(draws), shape[dim] // shards_of).reshape((-1,) + (1,) * (len(shape) - 1 - dim))
    return gain


def routed_block(rng, own, number, rows, count, top, most, slope):
    sequence = jax.random.permutation(rng, count)
    crowded, ordinary = load_shares(count, rows * top, most, slope, True), load_shares(count, rows * top, most, slope, False)
    places = jnp.arange(count)

    def named(lengths, turn):
        used = int((lengths > 0).sum())
        fixed = max(1, used // 4)
        moved = fixed + (places - fixed + turn * (used - fixed)) % max(1, count - fixed)
        return jnp.zeros((count,), jnp.int32).at[sequence[jnp.where(places < fixed, places, moved)]].set(jnp.asarray(lengths, jnp.int32))

    lengths = jnp.where(number % 4 == 0, named(crowded, number // 4), named(ordinary, number - number // 4 - 1))
    mixed = jax.random.permutation(jax.random.fold_in(own, 3), count)
    source_of, sink = mixed[0:count // 2 * 2:2], mixed[1:count // 2 * 2:2]
    room = jnp.minimum(lengths[source_of] - 1, most - lengths[sink]) // 2
    room = jnp.where((source_of == sequence[0]) | (sink == sequence[0]) | (lengths[sink] == 0), 0, jnp.maximum(room, 0))
    moved = jax.random.randint(jax.random.fold_in(own, 4), (count // 2,), 0, 1 << 20) % (room + 1)
    lengths = lengths.at[source_of].add(-moved).at[sink].add(moved)
    members = jnp.searchsorted(jnp.cumsum(lengths), jnp.arange(rows * top), side="right").astype(jnp.int32)
    listing = members.reshape(top, rows).T
    listing = listing[jax.random.permutation(jax.random.fold_in(own, 1), rows)]
    turn = jax.random.randint(jax.random.fold_in(own, 2), (rows, 1), 0, top)
    return jnp.take_along_axis(listing, (jnp.arange(top)[None, :] + turn) % top, axis=1)


def load_shares(count, total, bound, lean, full):
    weights = [(1 << 20) // math.isqrt(standing ** lean) + 1 for standing in range(1, count + 1)]
    largest = bound if full else min(bound, max(-(-total // count), total * weights[0] // sum(weights)))
    least = 1 if total - largest >= count - 1 else 0
    counts, rest = [largest] + [least] * (count - 1), total - largest - least * (count - 1)
    while rest > 0:
        free = [i for i in range(1, count) if counts[i] < largest] or [i for i in range(1, count) if counts[i] < bound]
        pool, budget = sum([weights[i] for i in free]), rest
        for i in free:
            more = min(bound - counts[i], max(1, budget * weights[i] // pool), rest)
            counts[i] = counts[i] + more
            rest = rest - more
    return np.array(counts)


def noise(key, extent, spread, most, split=(), kind=jnp.bfloat16):
    entries = jax.random.normal(key, extent, jnp.float32) * spread
    if len(split) > 0:
        entries = shard_levels(key, extent, split, -0.22, 0.18) * entries
    return jnp.clip(entries, min=-most, max=most).astype(kind)


def setup_inputs(seed: int = 0) -> dict:
    streams_of = jax.random.split(jax.random.key(seed), 8)
    tokens = noise(streams_of[0], (TOKENS, D), 1.0, 6.0, ((0, 32), (1, 8)))
    cotangent = noise(streams_of[1], (TOKENS, D), 1.0, 6.0, ((0, 32), (1, 8)))
    experts_keys = jax.random.split(jax.random.fold_in(streams_of[2], 1), TOKENS // TOK_DEV)
    experts_turns = jax.random.permutation(jax.random.fold_in(streams_of[2], 3), TOKENS // TOK_DEV)
    experts = jax.vmap(lambda own, number: routed_block(jax.random.fold_in(streams_of[2], 2), own, number, TOK_DEV, EXPERTS, TOP, CAP, 2))(experts_keys, experts_turns).reshape((TOKENS, TOP))
    gates = jnp.clip(0.1 + 0.79999997 * jax.random.uniform(streams_of[3], (TOKENS, TOP), jnp.float32) ** shard_levels(streams_of[3], (TOKENS, TOP), ((0, 32),), -0.2, 0.2), 0.1, 0.9)
    w_gate = noise(streams_of[4], (N_EXP, D, FF // GROUP), D ** -0.5, 0.09375, ((0, 32), (2, 8)))
    w_up = noise(streams_of[5], (N_EXP, D, FF // GROUP), D ** -0.5, 0.09375, ((0, 32), (2, 8)))
    w_down = noise(streams_of[6], (N_EXP, FF // GROUP, D), FF ** -0.5, 0.0625, ((0, 32), (1, 8)))
    return dict(tokens=tokens, cotangent=cotangent, experts=experts, gates=gates, w_gate=w_gate, w_up=w_up, w_down=w_down)


def slot_places(experts):
    pair_ids = experts.reshape(N_EXP, TOK_DEV * TOP)
    matches = (pair_ids[:, :, None] == jnp.arange(EXPERTS, dtype=jnp.int32)[None, None, :]).astype(jnp.int32)
    before = jnp.cumsum(matches, axis=1) - matches
    slot_ids = jnp.sum(before * matches, axis=2)
    source = jnp.arange(N_EXP, dtype=jnp.int32)[:, None] * CAP
    return (source + slot_ids).reshape(TOKENS * TOP).astype(jnp.int32)


def reference(tokens, cotangent, experts, gates, w_gate, w_up, w_down):
    places = slot_places(experts)
    expert_ids = experts.reshape(TOKENS * TOP).astype(jnp.int32)
    buffer_rows = N_EXP * CAP
    repeated = jnp.repeat(tokens, TOP, axis=0)
    scaled = (gates[:, :, None] * cotangent[:, None, :].astype(jnp.float32)).astype(jnp.bfloat16)
    scaled = scaled.reshape(TOKENS * TOP, D)
    part = FF // GROUP
    gate_all = w_gate.reshape(EXPERTS, GROUP, D, part).transpose(0, 2, 1, 3).reshape(EXPERTS, D, FF)
    up_all = w_up.reshape(EXPERTS, GROUP, D, part).transpose(0, 2, 1, 3).reshape(EXPERTS, D, FF)
    down_all = w_down.reshape(EXPERTS, FF, D)

    def expert_pass(expert):
        targets = jnp.where(expert_ids == expert, places, buffer_rows).astype(jnp.int32)
        token_rows = jnp.zeros((buffer_rows, D), jnp.bfloat16).at[targets].set(repeated, mode="drop")
        cot_rows = jnp.zeros((buffer_rows, D), jnp.bfloat16).at[targets].set(scaled, mode="drop")
        gate_mat = gate_all[expert]
        up_mat = up_all[expert]
        down_mat = down_all[expert]
        hidden_gate = jnp.dot(token_rows, gate_mat, preferred_element_type=jnp.float32)
        hidden_up = jnp.dot(token_rows, up_mat, preferred_element_type=jnp.float32)
        sigmoid_gate = jax.nn.sigmoid(hidden_gate)
        activation = (hidden_gate * sigmoid_gate * hidden_up).astype(jnp.bfloat16)
        out_rows = jnp.dot(activation, down_mat, preferred_element_type=jnp.float32)
        grad_act = jnp.dot(cot_rows, down_mat.T, preferred_element_type=jnp.float32)
        grad_first = (grad_act * hidden_up * sigmoid_gate * (1.0 + hidden_gate * (1.0 - sigmoid_gate))).astype(jnp.bfloat16)
        grad_second = (grad_act * hidden_gate * sigmoid_gate).astype(jnp.bfloat16)
        grad_down = jnp.dot(activation.T, cot_rows, preferred_element_type=jnp.float32).astype(jnp.bfloat16)
        grad_gate = jnp.dot(token_rows.T, grad_first, preferred_element_type=jnp.float32).astype(jnp.bfloat16)
        grad_up = jnp.dot(token_rows.T, grad_second, preferred_element_type=jnp.float32).astype(jnp.bfloat16)
        back_rows = jnp.dot(grad_first, gate_mat.T, preferred_element_type=jnp.float32)
        back_rows = back_rows + jnp.dot(grad_second, up_mat.T, preferred_element_type=jnp.float32)
        return out_rows, back_rows, grad_gate, grad_up, grad_down

    results = lax.map(expert_pass, jnp.arange(EXPERTS, dtype=jnp.int32))
    flat = (expert_ids * buffer_rows + places).astype(jnp.int32)
    out_pairs = results[0].reshape(EXPERTS * buffer_rows, D)[flat].reshape(TOKENS, TOP, D)
    back_pairs = results[1].reshape(EXPERTS * buffer_rows, D)[flat].reshape(TOKENS, TOP, D)
    output = jnp.sum(gates[:, :, None] * out_pairs, axis=1).astype(jnp.bfloat16)
    input_grad = jnp.sum(back_pairs, axis=1).astype(jnp.bfloat16)
    grad_gate = results[2].reshape(EXPERTS, D, GROUP, part).transpose(0, 2, 1, 3).reshape(N_EXP, D, part)
    grad_up = results[3].reshape(EXPERTS, D, GROUP, part).transpose(0, 2, 1, 3).reshape(N_EXP, D, part)
    grad_down = results[4].reshape(N_EXP, part, D)
    return output, input_grad, grad_gate, grad_up, grad_down
```

```python
import functools

import jax
import jax.numpy as jnp
from jax import lax
from jax.experimental import pallas as pl
from jax.experimental.pallas import tpu as pltpu
from jax.sharding import Mesh, PartitionSpec as P


EXPERTS = 8
CAP = 8
FBLK = 512
EXP_AXES = ("x", "yh", "yl", "c")
F32, BF16 = jnp.float32, jnp.bfloat16


def mm(a, b):
    return jnp.dot(a, b, preferred_element_type=F32)


def mm_nt(a, b):
    return lax.dot_general(a, b, (((1,), (1,)), ((), ())), preferred_element_type=F32)


def mm_tn(a, b):
    return lax.dot_general(a, b, (((0,), (0,)), ((), ())), preferred_element_type=F32)


def slot_hits(exp_ref, gate_ref, rows, group):
    n_tok = exp_ref.shape[1]
    r = lax.broadcasted_iota(jnp.int32, (rows, n_tok), 0)
    k, s = r // group, r % CAP
    first, second = exp_ref[0:1, :] == k, exp_ref[1:2, :] == k
    named = (first | second).astype(F32)
    before_of = lax.broadcasted_iota(jnp.int32, (n_tok, n_tok), 0) < lax.broadcasted_iota(
        jnp.int32, (n_tok, n_tok), 1
    )
    before = mm(named.astype(BF16), before_of.astype(F32).astype(BF16))
    hit = jnp.where(before == s.astype(F32), named, 0.0)
    gate = jnp.where(first, gate_ref[0:1, :], 0.0) + jnp.where(second, gate_ref[1:2, :], 0.0)
    return hit, hit * gate


def lane_shift(n_tok, by):
    row = lax.broadcasted_iota(jnp.int32, (n_tok, 2 * n_tok), 0)
    lane = lax.broadcasted_iota(jnp.int32, (n_tok, 2 * n_tok), 1)
    return (lane == row + by).astype(F32).astype(BF16)


def dispatch_kernel(exp_ref, gate_ref, in_ref, out_ref, *, yl):
    n_tok = exp_ref.shape[1]
    blocks, _, fblk = in_ref.shape
    hit, weighted = slot_hits(exp_ref, gate_ref, EXPERTS * CAP, CAP)
    hit = hit.astype(BF16)
    pick_x = mm(hit, lane_shift(n_tok, 0)).astype(BF16)
    pick_g = mm(hit, lane_shift(n_tok, n_tok)).astype(BF16)
    gate = jnp.sum(weighted, axis=1, keepdims=True)
    for b in range(blocks):
        x = mm(pick_x, in_ref[b])
        g = mm(pick_g, in_ref[b]) * gate
        for part, value in enumerate((x, g)):
            value = value.reshape(EXPERTS, CAP, fblk).astype(BF16)
            at = (part * blocks + b) * fblk
            for i in range(yl):
                out_ref[:, i, 0, :, at : at + fblk] = value


def hidden_kernel(c_ref, x_ref, g_ref, w1_ref, w3_ref, w2_ref, *refs, last):
    j, steps = pl.program_id(0), pl.num_programs(0)
    if last:
        i1, i3, ia, act_ref, d1_ref, d3_ref, h1, h3, da = refs
    else:
        h1, h3, da = refs

    @pl.when(j == 0)
    def _():
        h1[...] = i1[...] if last else jnp.zeros_like(h1)
        h3[...] = i3[...] if last else jnp.zeros_like(h3)
        da[...] = ia[...] if last else jnp.zeros_like(da)

    x, g = x_ref[...], g_ref[...]
    h1[...] += mm(x, w1_ref[...])
    h3[...] += mm(x, w3_ref[...])
    da[...] += mm_nt(g, w2_ref[...])

    if last:

        @pl.when(j == steps - 1)
        def _():
            first, second, third = h1[...], h3[...], da[...]
            sig = jax.nn.sigmoid(first)
            act_ref[...] = (first * sig * second).astype(BF16)
            d1_ref[...] = (third * second * sig * (1.0 + first * (1.0 - sig))).astype(BF16)
            d3_ref[...] = (third * first * sig).astype(BF16)


def back_kernel(c_ref, act_ref, d1_ref, d3_ref, w1_ref, w3_ref, w2_ref, *refs, half):
    j = pl.program_id(0)
    out_ref = refs[-1]

    def put(value):
        if len(refs) == 2:
            value = value + refs[0][...].astype(F32)
        out_ref[...] = value.astype(BF16)

    @pl.when(j < half)
    def _():
        put(mm(act_ref[...], w2_ref[...]))

    @pl.when(j >= half)
    def _():
        put(mm_nt(d1_ref[...], w1_ref[...]) + mm_nt(d3_ref[...], w3_ref[...]))


def weight_grad_kernel(
    c_ref, x0_ref, g0_ref, x1_ref, g1_ref, act_ref, d1_ref, d3_ref, gg_ref, gu_ref, gd_ref, *, half
):
    j = pl.program_id(0)

    def put(x_ref, g_ref):
        x = x_ref[...]
        gg_ref[...] = mm_tn(x, d1_ref[...]).astype(BF16)
        gu_ref[...] = mm_tn(x, d3_ref[...]).astype(BF16)
        gd_ref[...] = mm_tn(act_ref[...], g_ref[...]).astype(BF16)

    @pl.when(j < half)
    def _():
        put(x0_ref, g0_ref)

    @pl.when(j >= half)
    def _():
        put(x1_ref, g1_ref)


def combine_kernel(exp_ref, gate_ref, y_ref, dx_ref, out_ref, *, yl):
    n_tok = exp_ref.shape[1]
    rows = EXPERTS * yl * CAP
    hit, weighted = slot_hits(exp_ref, gate_ref, rows, yl * CAP)
    high = weighted.astype(BF16)
    low = (weighted - high.astype(F32)).astype(BF16)
    left, right = lane_shift(n_tok, 0), lane_shift(n_tok, n_tok)
    y = y_ref[...].astype(F32).reshape(rows, y_ref.shape[-1]).astype(BF16)
    dx = dx_ref[...].astype(F32).reshape(rows, dx_ref.shape[-1]).astype(BF16)
    out = mm_tn(mm(high, left).astype(BF16), y) + mm_tn(mm(low, left).astype(BF16), y)
    out = out + mm_tn(mm(hit.astype(BF16), right).astype(BF16), dx)
    out_ref[0] = out.astype(BF16)


def call(kernel, name, grid, ins, outs, scratch=(), prefetch=0, flops=0, nbytes=0):
    return pl.pallas_call(
        kernel,
        name=name,
        grid_spec=pltpu.PrefetchScalarGridSpec(
            num_scalar_prefetch=prefetch,
            grid=grid,
            in_specs=[pl.BlockSpec(b, m) for b, m in ins],
            out_specs=[pl.BlockSpec(b, m) for _, b, m in outs],
            scratch_shapes=list(scratch),
        ),
        out_shape=[s for s, _, _ in outs],
        compiler_params=pltpu.CompilerParams(dimension_semantics=("arbitrary",)),
        cost_estimate=pl.CostEstimate(flops=flops, bytes_accessed=nbytes, transcendentals=0),
    )


def per_device(tokens, cotangent, experts, gates, w_gate, w_up, w_down):
    sizes = {a: lax.axis_size(a) for a in EXP_AXES + ("tp",)}
    n_exp = sizes["x"] * sizes["yh"] * sizes["yl"] * sizes["c"]
    yl, tp = sizes["yl"], sizes["tp"]
    n_tok, fblk = tokens.shape
    w1, w3, w2 = w_gate[0], w_up[0], w_down[0]
    width, hid = w1.shape
    half = tp // 2
    wide = half * fblk
    rows = n_exp * CAP
    core = lax.axis_index("c").astype(jnp.int32)
    own = core[None]
    other = 1 - own
    exp_t, gate_t = experts.T, gates.T

    both = jnp.concatenate([tokens, cotangent], axis=0)
    spread = jnp.broadcast_to(both[None], (tp,) + both.shape)
    mine = lax.all_to_all(spread, "tp", 0, 0, tiled=True)

    small = ((2, n_tok), lambda *_: (0, 0))
    (send,) = call(
        functools.partial(dispatch_kernel, yl=yl),
        "dispatch",
        (2,),
        [small, small, ((half, 2 * n_tok, fblk), lambda c: (c, 0, 0))],
        [
            (
                jax.ShapeDtypeStruct((EXPERTS, yl, 2, CAP, 2 * wide), BF16),
                (EXPERTS, yl, 1, CAP, 2 * wide),
                lambda c: (0, 0, c, 0, 0),
            )
        ],
    )(exp_t, gate_t, mine)
    send = send.reshape(n_exp, CAP, 2 * wide)
    got = lax.all_to_all(send, EXP_AXES, 0, 0, tiled=True)

    swap = [(0, 1), (1, 0)]
    got0 = got.reshape(rows, 2 * wide)
    got1 = lax.ppermute(got0, "c", swap)
    square = (rows, hid)
    whole = (square, lambda j, c: (0, 0))
    x_of = ((rows, fblk), lambda j, c: (0, j))
    g_of = ((rows, fblk), lambda j, c: (0, half + j))
    w_rows = ((fblk, hid), lambda j, c: (c[0] * half + j, 0))
    w_cols = ((hid, fblk), lambda j, c: (0, c[0] * half + j))
    as_f32 = (jax.ShapeDtypeStruct(square, F32), *whole)
    as_bf16 = (jax.ShapeDtypeStruct(square, BF16), *whole)
    product = 2 * rows * wide * hid
    moved = 2 * wide * (2 * rows + 3 * hid)
    ins = [x_of, g_of, w_rows, w_rows, w_cols]
    part = call(
        functools.partial(hidden_kernel, last=False),
        "hidden_own",
        (half,),
        ins,
        [as_f32] * 3,
        prefetch=1,
        flops=3 * product,
        nbytes=moved,
    )(own, got0, got0, w1, w3, w2)
    act, d1, d3 = call(
        functools.partial(hidden_kernel, last=True),
        "hidden_other",
        (half,),
        ins + [whole] * 3,
        [as_bf16] * 3,
        scratch=[pltpu.VMEM(square, F32)] * 3,
        prefetch=1,
        flops=3 * product,
        nbytes=moved,
    )(other, got1, got1, w1, w3, w2, *part)

    first_of = lambda j: jnp.minimum(j, half - 1)
    later_of = lambda j: jnp.maximum(j - half, 0)
    w_rows = ((fblk, hid), lambda j, c: (c[0] * half + later_of(j), 0))
    w_cols = ((hid, fblk), lambda j, c: (0, c[0] * half + first_of(j)))
    piece = ((rows, fblk), lambda j, c: (0, j))
    back = functools.partial(
        call,
        functools.partial(back_kernel, half=half),
        grid=(2 * half,),
        outs=[(jax.ShapeDtypeStruct((rows, 2 * wide), BF16), *piece)],
        prefetch=1,
        flops=3 * product,
        nbytes=moved,
    )
    ins = [whole] * 3 + [w_rows, w_rows, w_cols]
    (theirs,) = back(name="back_other", ins=ins)(other, act, d1, d3, w1, w3, w2)
    theirs = lax.ppermute(theirs, "c", swap)
    (ours,) = back(name="back_own", ins=ins + [piece])(own, act, d1, d3, w1, w3, w2, theirs)
    home = lax.all_to_all(ours.reshape(n_exp, CAP, 2 * wide), EXP_AXES, 0, 0, tiled=True)

    x0 = ((rows, fblk), lambda j, c: (0, first_of(j)))
    g0 = ((rows, fblk), lambda j, c: (0, half + first_of(j)))
    x1 = ((rows, fblk), lambda j, c: (0, later_of(j)))
    g1 = ((rows, fblk), lambda j, c: (0, half + later_of(j)))
    at = lambda j, c: lax.rem(c[0] * half + j, 2 * half)
    tall = ((fblk, hid), lambda j, c: (at(j, c), 0))
    flat = ((hid, fblk), lambda j, c: (0, at(j, c)))
    grad_gate, grad_up, grad_down = call(
        functools.partial(weight_grad_kernel, half=half),
        "weight_grad",
        (2 * half,),
        [x0, g0, x1, g1] + [whole] * 3,
        [
            (jax.ShapeDtypeStruct(w1.shape, BF16), *tall),
            (jax.ShapeDtypeStruct(w3.shape, BF16), *tall),
            (jax.ShapeDtypeStruct(w2.shape, BF16), *flat),
        ],
        prefetch=1,
        flops=6 * product,
        nbytes=4 * wide * (2 * rows + 3 * hid),
    )(own, got0, got0, got1, got1, act, d1, d3)

    home = home.reshape(EXPERTS, yl, 2, CAP, 2 * wide)
    shape = (EXPERTS, yl, 1, CAP, fblk)
    (mixed,) = call(
        functools.partial(combine_kernel, yl=yl),
        "combine",
        (tp,),
        [
            small,
            small,
            (shape, lambda t: (0, 0, t // half, 0, t % half)),
            (shape, lambda t: (0, 0, t // half, 0, half + t % half)),
        ],
        [
            (
                jax.ShapeDtypeStruct((tp, 2 * n_tok, fblk), BF16),
                (1, 2 * n_tok, fblk),
                lambda t: (t, 0, 0),
            )
        ],
    )(exp_t, gate_t, home, home)
    parts = lax.all_to_all(mixed, "tp", 0, 0, tiled=True)
    total = jnp.sum(parts.astype(F32), axis=0)
    output, input_grad = total[:n_tok].astype(BF16), total[n_tok:].astype(BF16)
    return output, input_grad, grad_gate[None], grad_up[None], grad_down[None]


def solution(mesh):
    group = mesh.shape["exp"] // EXPERTS
    x, yl = EXPERTS // 2, group // 2
    shape = (x, 2, yl, 2, mesh.shape["tp"])
    fine = Mesh(mesh.devices.reshape(shape), EXP_AXES + ("tp",))
    spec = (
        P(EXP_AXES, "tp"),
        P(EXP_AXES, "tp"),
        P(EXP_AXES, None),
        P(EXP_AXES, None),
        P(EXP_AXES, None, "tp"),
        P(EXP_AXES, None, "tp"),
        P(EXP_AXES, "tp", None),
    )
    out = (spec[0], spec[1], spec[4], spec[5], spec[6])
    return jax.shard_map(per_device, mesh=fine, in_specs=spec, out_specs=out, check_vma=False)
```

```python
import functools
import math

import jax
import jax.numpy as jnp
from jax import lax
from jax.experimental import pallas as pl
from jax.experimental.pallas import tpu as pltpu
from jax.sharding import Mesh, PartitionSpec as P


EXPERTS = 8
CAP = 8

EXP_AXES = ("x", "yh", "yl", "c")
TP_AXES = ("za", "zb")
PEERS = ("zb", "x", "yh", "yl")
F32, BF16 = jnp.float32, jnp.bfloat16


def mm(a, b):
    return jnp.dot(a, b, preferred_element_type=F32)


def mm_nt(a, b):
    return lax.dot_general(a, b, (((1,), (1,)), ((), ())), preferred_element_type=F32)


def mm_tn(a, b):
    return lax.dot_general(a, b, (((0,), (0,)), ((), ())), preferred_element_type=F32)


def slot_hits(exp_ref, gate_ref, rows, group):
    n_tok = exp_ref.shape[1]
    r = lax.broadcasted_iota(jnp.int32, (rows, n_tok), 0)
    k, s = r // group, r % CAP
    first, second = exp_ref[0:1, :] == k, exp_ref[1:2, :] == k
    named = (first | second).astype(F32)
    before_of = lax.broadcasted_iota(jnp.int32, (n_tok, n_tok), 0) < lax.broadcasted_iota(
        jnp.int32, (n_tok, n_tok), 1
    )
    before = mm(named.astype(BF16), before_of.astype(F32).astype(BF16))
    hit = jnp.where(before == s.astype(F32), named, 0.0)
    gate = jnp.where(first, gate_ref[0:1, :], 0.0) + jnp.where(second, gate_ref[1:2, :], 0.0)
    return hit, hit * gate


def lane_shift(n_tok, by):
    row = lax.broadcasted_iota(jnp.int32, (n_tok, 2 * n_tok), 0)
    lane = lax.broadcasted_iota(jnp.int32, (n_tok, 2 * n_tok), 1)
    return (lane == row + by).astype(F32).astype(BF16)


def route_kernel(exp_ref, gate_ref, x_ref, g_ref, scale_ref, high_ref, low_ref, hit_ref, *, group):
    n_tok = exp_ref.shape[1]
    left, right = lane_shift(n_tok, 0), lane_shift(n_tok, n_tok)
    hit, weighted = slot_hits(exp_ref, gate_ref, EXPERTS * CAP, CAP)
    x_ref[...] = mm(hit.astype(BF16), left).astype(BF16)
    g_ref[...] = mm(hit.astype(BF16), right).astype(BF16)
    scale_ref[...] = jnp.broadcast_to(jnp.sum(weighted, axis=1, keepdims=True), scale_ref.shape)

    rows = EXPERTS * group
    hit, weighted = slot_hits(exp_ref, gate_ref, rows, group)
    high = weighted.astype(BF16)
    low = (weighted - high.astype(F32)).astype(BF16)
    same = (
        lax.broadcasted_iota(jnp.int32, (rows, rows), 0)
        == lax.broadcasted_iota(jnp.int32, (rows, rows), 1)
    )
    same = same.astype(F32).astype(BF16)
    for ref, table, side in ((high_ref, high, left), (low_ref, low, left), (hit_ref, hit, right)):
        ref[...] = mm_tn(mm(table.astype(BF16), side).astype(BF16), same).astype(BF16)


def dispatch_kernel(x_ref, g_ref, scale_ref, in_ref, out_ref):
    zb, _, yl, _, _ = out_ref.shape
    blocks, _, fblk = in_ref.shape
    for b in range(blocks):
        x = mm(x_ref[...], in_ref[b])
        g = mm(g_ref[...], in_ref[b]) * scale_ref[:, :1]
        for part, value in enumerate((x, g)):
            value = value.reshape(EXPERTS, CAP, fblk).astype(BF16)
            at = (part * blocks + b) * fblk
            for i in range(zb):
                for j in range(yl):
                    out_ref[i, :, j, :, at : at + fblk] = value


def hidden(got_ref, w1_ref, w3_ref, w2_ref, act_ref, d1_ref, d3_ref, fblk):
    pairs, _, wide = got_ref.shape
    half = wide // 2
    first = second = third = 0.0
    for p in range(pairs):
        for b in range(half // fblk):
            x = got_ref[p, :, b * fblk : (b + 1) * fblk]
            g = got_ref[p, :, half + b * fblk : half + (b + 1) * fblk]
            at = (b * pairs + p) * fblk
            first = first + mm(x, w1_ref[at : at + fblk, :])
            second = second + mm(x, w3_ref[at : at + fblk, :])
            third = third + mm_nt(g, w2_ref[:, at : at + fblk])
    sig = jax.nn.sigmoid(first)
    act_ref[...] = (first * sig * second).astype(BF16)
    d1_ref[...] = (third * second * sig * (1.0 + first * (1.0 - sig))).astype(BF16)
    d3_ref[...] = (third * first * sig).astype(BF16)


def back_x(d1_ref, d3_ref, w1_ref, w3_ref, out_ref, fblk):
    pairs, _, wide = out_ref.shape
    for p in range(pairs):
        for b in range(wide // fblk):
            at = (b * pairs + p) * fblk
            value = mm_nt(d1_ref[...], w1_ref[at : at + fblk, :])
            value = value + mm_nt(d3_ref[...], w3_ref[at : at + fblk, :])
            out_ref[p, :, b * fblk : (b + 1) * fblk] = value.astype(BF16)


def back_y(act_ref, w2_ref, out_ref, fblk):
    pairs, _, wide = out_ref.shape
    for p in range(pairs):
        for b in range(wide // fblk):
            at = (b * pairs + p) * fblk
            value = mm(act_ref[...], w2_ref[:, at : at + fblk])
            out_ref[p, :, b * fblk : (b + 1) * fblk] = value.astype(BF16)


def own_kernel(got, w1, w3, w2, act, d1, d3, y, dx, *, fblk):
    hidden(got, w1, w3, w2, act, d1, d3, fblk)
    back_y(act, w2, y, fblk)
    back_x(d1, d3, w1, w3, dx, fblk)


def other_y_kernel(got, w1, w3, w2, _, act, d1, d3, y, *, fblk):
    hidden(got, w1, w3, w2, act, d1, d3, fblk)
    back_y(act, w2, y, fblk)


def other_x_kernel(d1, d3, w1, w3, dx, *, fblk):
    back_x(d1, d3, w1, w3, dx, fblk)


def add_kernel(y0, y1, dx0, dx1, out_ref, total, sems):
    pairs, _, wide = y0.shape
    copies = []
    for part, (mine, theirs) in enumerate(((y0, y1), (dx0, dx1))):
        for p in range(pairs):
            lanes = slice(part * wide, (part + 1) * wide)
            total[p, :, lanes] = (mine[p].astype(F32) + theirs[p].astype(F32)).astype(BF16)
            copies.append(
                pltpu.make_async_copy(
                    total.at[p, :, lanes], out_ref.at[p, :, lanes], sems.at[part * pairs + p]
                )
            )
            copies[-1].start()
    for copy in copies:
        copy.wait()


def weight_grad_kernel(got0, got1, a0, a1, b0, b1, c0, c1, gg_ref, gu_ref, gd_ref, done_ref):
    t = pl.program_id(0)
    pairs, _, wide = got0.shape
    fblk = gg_ref.shape[0]
    p, b = lax.rem(t, pairs), lax.div(t, pairs)
    x_at = pl.ds(pl.multiple_of(b * fblk, fblk), fblk)
    g_at = pl.ds(pl.multiple_of(wide // 2 + b * fblk, fblk), fblk)
    both = lambda u, v: jnp.concatenate([u, v], axis=0)
    x = both(got0[p, :, x_at], got1[p, :, x_at])
    g = both(got0[p, :, g_at], got1[p, :, g_at])
    gg_ref[...] = mm_tn(x, both(b0[...], b1[...])).astype(BF16)
    gu_ref[...] = mm_tn(x, both(c0[...], c1[...])).astype(BF16)
    gd_ref[...] = mm_tn(both(a0[...], a1[...]), g).astype(BF16)
    done_ref[...] = jnp.zeros_like(done_ref)


def combine_kernel(high_ref, low_ref, hit_ref, home_ref, _, out_ref):
    pairs, _, wide = home_ref.shape
    blocks, _, fblk = out_ref.shape
    for b in range(blocks):
        out = 0.0
        for p in range(pairs):
            y = home_ref[p, :, b * fblk : (b + 1) * fblk]
            dx = home_ref[p, :, wide // 2 + b * fblk : wide // 2 + (b + 1) * fblk]
            out = out + mm(high_ref[...], y) + mm(low_ref[...], y) + mm(hit_ref[...], dx)
        out_ref[b] = out.astype(BF16)


VMEM = pl.BlockSpec(memory_space=pltpu.VMEM)
HBM = pl.BlockSpec(memory_space=pltpu.HBM)


def call(kernel, ins, outs, grid=(), out_specs=None, scratch=(), flops=0, nbytes=0):
    return pl.pallas_call(
        kernel,
        grid=grid,
        in_specs=[VMEM] * ins if isinstance(ins, int) else ins,
        out_specs=out_specs or [VMEM] * len(outs),
        out_shape=[jax.ShapeDtypeStruct(shape, dtype) for shape, dtype in outs],
        scratch_shapes=list(scratch),
        compiler_params=pltpu.CompilerParams(vmem_limit_bytes=24 * 1024 * 1024),
        cost_estimate=pl.CostEstimate(flops=flops, bytes_accessed=nbytes, transcendentals=0),
    )


def per_device(tokens, cotangent, experts, gates, w_gate, w_up, w_down):
    za, zb, yl = (lax.axis_size(a) for a in ("za", "zb", "yl"))
    peers = math.prod(lax.axis_size(a) for a in PEERS)
    n_tok, fblk = tokens.shape
    w1, w3, w2 = w_gate[0], w_up[0], w_down[0]
    width, hid = w1.shape
    wide = za * fblk
    rows = peers // zb * CAP
    swap = [(0, 1), (1, 0)]
    fb = dict(fblk=fblk)

    both = jnp.concatenate([tokens, cotangent], axis=0)
    spread = jnp.broadcast_to(both[None], (za,) + both.shape)
    mine = lax.all_to_all(spread, "za", 0, 0, tiled=True)
    table = ((2 * n_tok, EXPERTS * yl * CAP), BF16)
    pick = ((EXPERTS * CAP, 2 * n_tok), BF16)
    pick_x, pick_g, scale, high, low, hit = call(
        functools.partial(route_kernel, group=yl * CAP),
        2,
        [pick, pick, ((EXPERTS * CAP, 128), F32)] + [table] * 3,
    )(experts.T, gates.T)

    (send,) = call(dispatch_kernel, 4, [((zb, EXPERTS, yl, CAP, 2 * wide), BF16)])(
        pick_x, pick_g, scale, mine
    )
    send = send.reshape(peers, CAP, 2 * wide)
    got0 = lax.all_to_all(send, PEERS, 0, 0, tiled=True).reshape(zb, rows, 2 * wide)

    got1 = lax.ppermute(got0, "c", swap)
    product = 2 * rows * width * hid
    square = [((rows, hid), BF16)] * 3
    piece = ((zb, rows, wide), BF16)
    a0, b0, c0, y0, dx0 = call(
        functools.partial(own_kernel, **fb), 4, square + [piece] * 2, flops=6 * product
    )(got0, w1, w3, w2)
    a1, b1, c1, y1 = call(
        functools.partial(other_y_kernel, **fb), 5, square + [piece], flops=4 * product
    )(got1, w1, w3, w2, a0)
    y1 = lax.ppermute(y1, "c", swap)
    (dx1,) = call(
        functools.partial(other_x_kernel, **fb), 4, [piece], flops=2 * product
    )(b1, c1, w1, w3)
    dx1 = lax.ppermute(dx1, "c", swap)

    full = (zb, rows, 2 * wide)
    (ours,) = call(
        add_kernel,
        4,
        [(full, BF16)],
        out_specs=[HBM],
        scratch=[pltpu.VMEM(full, BF16), pltpu.SemaphoreType.DMA((2 * zb,))],
    )(y0, y1, dx0, dx1)
    home = lax.all_to_all(ours.reshape(peers, CAP, 2 * wide), PEERS, 0, 0, tiled=True)

    tall = pl.BlockSpec((fblk, hid), lambda t: (t, 0))
    flat = pl.BlockSpec((hid, fblk), lambda t: (0, t))
    grad_gate, grad_up, grad_down, done = call(
        weight_grad_kernel,
        8,
        [((width, hid), BF16)] * 2 + [((hid, width), BF16), ((8, 128), F32)],
        grid=(width // fblk,),
        out_specs=[tall, tall, flat, pl.BlockSpec((8, 128), lambda t: (0, 0))],
        flops=6 * product,
        nbytes=6 * width * hid,
    )(got0, got1, a0, a1, b0, b1, c0, c1)

    (mixed,) = call(combine_kernel, 5, [((za, 2 * n_tok, fblk), BF16)])(
        high, low, hit, home.reshape(zb, EXPERTS * yl * CAP, 2 * wide), done
    )
    parts = lax.all_to_all(mixed, "za", 0, 0, tiled=True)
    total = jnp.sum(parts.astype(F32), axis=0)
    output, input_grad = total[:n_tok].astype(BF16), total[n_tok:].astype(BF16)
    return output, input_grad, grad_gate[None], grad_up[None], grad_down[None]


def solution(mesh):
    group = mesh.shape["exp"] // EXPERTS
    shape = (EXPERTS // 2, 2, group // 2, 2, mesh.shape["tp"] // 2, 2)
    fine = Mesh(mesh.devices.reshape(shape), EXP_AXES + TP_AXES)
    spec = (
        P(EXP_AXES, TP_AXES),
        P(EXP_AXES, TP_AXES),
        P(EXP_AXES, None),
        P(EXP_AXES, None),
        P(EXP_AXES, None, TP_AXES),
        P(EXP_AXES, None, TP_AXES),
        P(EXP_AXES, TP_AXES, None),
    )
    out = (spec[0], spec[1], spec[4], spec[5], spec[6])
    return jax.shard_map(per_device, mesh=fine, in_specs=spec, out_specs=out, check_vma=False)
```

```python
import functools
import math

import jax
import jax.numpy as jnp
from jax import lax
from jax.experimental import pallas as pl
from jax.experimental.pallas import tpu as pltpu
from jax.sharding import Mesh, PartitionSpec as P


EXPERTS = 8
CAP = 8

EXP_AXES = ("x", "yh", "yl", "c")
TP_AXES = ("za", "zb")
PEERS = ("zb", "x", "yh", "yl")
F32, BF16 = jnp.float32, jnp.bfloat16


def mm(a, b):
    return jnp.dot(a, b, preferred_element_type=F32)


def mm_nt(a, b):
    return lax.dot_general(a, b, (((1,), (1,)), ((), ())), preferred_element_type=F32)


def mm_tn(a, b):
    return lax.dot_general(a, b, (((0,), (0,)), ((), ())), preferred_element_type=F32)


def slot_hits(exp_ref, gate_ref, rows, group):
    n_tok = exp_ref.shape[1]
    r = lax.broadcasted_iota(jnp.int32, (rows, n_tok), 0)
    k, s = r // group, r % CAP
    first, second = exp_ref[0:1, :] == k, exp_ref[1:2, :] == k
    named = (first | second).astype(F32)
    before_of = lax.broadcasted_iota(jnp.int32, (n_tok, n_tok), 0) < lax.broadcasted_iota(
        jnp.int32, (n_tok, n_tok), 1
    )
    before = mm(named.astype(BF16), before_of.astype(F32).astype(BF16))
    hit = jnp.where(before == s.astype(F32), named, 0.0)
    gate = jnp.where(first, gate_ref[0:1, :], 0.0) + jnp.where(second, gate_ref[1:2, :], 0.0)
    return hit, hit * gate


def lane_shift(n_tok, by):
    row = lax.broadcasted_iota(jnp.int32, (n_tok, 2 * n_tok), 0)
    lane = lax.broadcasted_iota(jnp.int32, (n_tok, 2 * n_tok), 1)
    return (lane == row + by).astype(F32).astype(BF16)


def route_kernel(exp_ref, gate_ref, x_ref, g_ref, scale_ref, high_ref, low_ref, hit_ref, *, group):
    n_tok = exp_ref.shape[1]
    left, right = lane_shift(n_tok, 0), lane_shift(n_tok, n_tok)
    hit, weighted = slot_hits(exp_ref, gate_ref, EXPERTS * CAP, CAP)
    x_ref[...] = mm(hit.astype(BF16), left).astype(BF16)
    g_ref[...] = mm(hit.astype(BF16), right).astype(BF16)
    scale_ref[...] = jnp.broadcast_to(jnp.sum(weighted, axis=1, keepdims=True), scale_ref.shape)

    rows = EXPERTS * group
    hit, weighted = slot_hits(exp_ref, gate_ref, rows, group)
    high = weighted.astype(BF16)
    low = (weighted - high.astype(F32)).astype(BF16)
    same = (
        lax.broadcasted_iota(jnp.int32, (rows, rows), 0)
        == lax.broadcasted_iota(jnp.int32, (rows, rows), 1)
    )
    same = same.astype(F32).astype(BF16)
    for ref, table, side in ((high_ref, high, left), (low_ref, low, left), (hit_ref, hit, right)):
        ref[...] = mm_tn(mm(table.astype(BF16), side).astype(BF16), same).astype(BF16)


def dispatch_kernel(x_ref, g_ref, scale_ref, in_ref, out_ref, rows, sems):
    zb, _, yl, _, _ = out_ref.shape
    blocks, _, fblk = in_ref.shape
    copies = []
    for part, pick in enumerate((x_ref, g_ref)):
        for b in range(blocks):
            value = mm(pick[...], in_ref[b])
            if part:
                value = value * scale_ref[:, :1]
            at = (part * blocks + b) * fblk
            rows[:, :, at : at + fblk] = value.reshape(EXPERTS, CAP, fblk).astype(BF16)
        lanes = slice(part * blocks * fblk, (part + 1) * blocks * fblk)
        for i in range(zb):
            for j in range(yl):
                copies.append(
                    pltpu.make_async_copy(
                        rows.at[:, :, lanes], out_ref.at[i, :, j, :, lanes], sems.at[len(copies)]
                    )
                )
                copies[-1].start()
    for copy in copies:
        copy.wait()


def rows_kernel(got, w1, w3, w2, v1, v3, v2, acts, their_acts, out_ref, up, down, total, in_sems, sems):
    pairs, rows, wide = got.shape
    half, hid = wide // 2, w1.shape[1]
    steps = in_sems.shape[0]
    fblk = w1.shape[0] // steps
    loads = []
    for t in range(steps):
        span = slice(t * fblk, (t + 1) * fblk)
        block = [
            pltpu.make_async_copy(w.at[span], up.at[span, i * hid : (i + 1) * hid], in_sems.at[t, i])
            for i, w in enumerate((w1, v1, w3, v3))
        ]
        block += [
            pltpu.make_async_copy(
                w.at[:, span], down.at[i * hid : (i + 1) * hid, span], in_sems.at[t, 4 + i]
            )
            for i, w in enumerate((w2, v2))
        ]
        for load in block:
            load.start()
        loads.append(block)

    first = second = third = 0.0
    for t in range(steps):
        for load in loads[t]:
            load.wait()
        p, at = t % pairs, t // pairs * fblk
        span = slice(t * fblk, (t + 1) * fblk)
        x, g = got[p, :, at : at + fblk], got[p, :, half + at : half + at + fblk]
        first = first + mm(x, up[span, : 2 * hid])
        second = second + mm(x, up[span, 2 * hid :])
        third = third + mm_nt(g, down[:, span])
    sig = jax.nn.sigmoid(first)
    act = (first * sig * second).astype(BF16)
    d1 = (third * second * sig * (1.0 + first * (1.0 - sig))).astype(BF16)
    d3 = (third * first * sig).astype(BF16)
    for i, value in enumerate((act, d1, d3)):
        acts[i] = value[:, :hid]
        their_acts[i] = value[:, hid:]
    both = jnp.concatenate([d1, d3], axis=1)

    copies = []
    cut = fblk // 2
    for t in range(steps):
        p, at = t % pairs, t // pairs * fblk
        for i in range(2):
            span = slice(t * fblk + i * cut, t * fblk + (i + 1) * cut)
            here = at + i * cut
            total[p, :, here : here + cut] = mm(act, down[:, span]).astype(BF16)
            total[p, :, half + here : half + here + cut] = mm_nt(both, up[span, :]).astype(BF16)
        for base in (0, half):
            lanes = slice(base + at, base + at + fblk)
            copies.append(
                pltpu.make_async_copy(
                    total.at[p, :, lanes], out_ref.at[p, :, lanes], sems.at[len(copies)]
                )
            )
            copies[-1].start()
    for copy in copies:
        copy.wait()


def weight_grad_kernel(got0, got1, acts0, acts1, gg_ref, gu_ref, gd_ref, done_ref):
    t = pl.program_id(0)
    pairs, _, wide = got0.shape
    fblk = gg_ref.shape[0]
    p, b = lax.rem(t, pairs), lax.div(t, pairs)
    x_at = pl.ds(pl.multiple_of(b * fblk, fblk), fblk)
    g_at = pl.ds(pl.multiple_of(wide // 2 + b * fblk, fblk), fblk)
    x = jnp.concatenate([got0[p, :, x_at], got1[p, :, x_at]], axis=0)
    g = jnp.concatenate([got0[p, :, g_at], got1[p, :, g_at]], axis=0)
    act, d1, d3 = (jnp.concatenate([acts0[i], acts1[i]], axis=0) for i in range(3))
    gg_ref[...] = mm_tn(x, d1).astype(BF16)
    gu_ref[...] = mm_tn(x, d3).astype(BF16)
    gd_ref[...] = mm_tn(act, g).astype(BF16)
    done_ref[...] = jnp.zeros_like(done_ref)


def combine_kernel(high_ref, low_ref, hit_ref, home_ref, _, out_ref):
    pairs, _, wide = home_ref.shape
    blocks, _, fblk = out_ref.shape
    for b in range(blocks):
        out = 0.0
        for p in range(pairs):
            y = home_ref[p, :, b * fblk : (b + 1) * fblk]
            dx = home_ref[p, :, wide // 2 + b * fblk : wide // 2 + (b + 1) * fblk]
            out = out + mm(high_ref[...], y) + mm(low_ref[...], y) + mm(hit_ref[...], dx)
        out_ref[b] = out.astype(BF16)


VMEM = pl.BlockSpec(memory_space=pltpu.VMEM)
HBM = pl.BlockSpec(memory_space=pltpu.HBM)


def call(kernel, name, ins, outs, grid=(), out_specs=None, scratch=(), mib=8, flops=0, nbytes=0):
    out_specs = out_specs or [VMEM] * len(outs)
    return pl.pallas_call(
        kernel,
        name=name,
        grid=grid,
        in_specs=[VMEM] * ins if isinstance(ins, int) else ins,
        out_specs=out_specs,
        out_shape=[
            (pltpu.HBM if spec is HBM else jax.ShapeDtypeStruct)(shape, dtype)
            for (shape, dtype), spec in zip(outs, out_specs)
        ],
        scratch_shapes=list(scratch),
        compiler_params=pltpu.CompilerParams(vmem_limit_bytes=mib * 1024 * 1024),
        cost_estimate=pl.CostEstimate(flops=flops, bytes_accessed=nbytes, transcendentals=0),
    )


def per_device(tokens, cotangent, experts, gates, w_gate, w_up, w_down):
    za, zb, yl = (lax.axis_size(a) for a in ("za", "zb", "yl"))
    peers = math.prod(lax.axis_size(a) for a in PEERS)
    n_tok, fblk = tokens.shape
    w1, w3, w2 = w_gate[0], w_up[0], w_down[0]
    width, hid = w1.shape
    wide = za * fblk
    rows = peers // zb * CAP
    swap = [(0, 1), (1, 0)]
    v1, v3, v2 = (lax.ppermute(w, "c", swap) for w in (w1, w3, w2))

    both = jnp.concatenate([tokens, cotangent], axis=0)
    spread = jnp.broadcast_to(both[None], (za,) + both.shape)
    mine = lax.all_to_all(spread, "za", 0, 0, tiled=True)
    table = ((2 * n_tok, EXPERTS * yl * CAP), BF16)
    pick = ((EXPERTS * CAP, 2 * n_tok), BF16)
    pick_x, pick_g, scale, high, low, hit = call(
        functools.partial(route_kernel, group=yl * CAP),
        "route",
        2,
        [pick, pick, ((EXPERTS * CAP, 128), F32)] + [table] * 3,
    )(experts.T, gates.T)

    (send,) = call(
        dispatch_kernel,
        "dispatch",
        4,
        [((zb, EXPERTS, yl, CAP, 2 * wide), BF16)],
        out_specs=[HBM],
        scratch=[
            pltpu.VMEM((EXPERTS, CAP, 2 * wide), BF16),
            pltpu.SemaphoreType.DMA((2 * zb * yl,)),
        ],
    )(pick_x, pick_g, scale, mine)
    send = send.reshape(peers, CAP, 2 * wide)
    got0 = lax.all_to_all(send, PEERS, 0, 0, tiled=True).reshape(zb, rows, 2 * wide)

    product = 2 * rows * width * hid
    acts, their_acts, ours = call(
        rows_kernel,
        "rows",
        [VMEM] + [HBM] * 6,
        [((3, rows, hid), BF16)] * 2 + [((zb, rows, 2 * wide), BF16)],
        out_specs=[VMEM, VMEM, HBM],
        scratch=[
            pltpu.VMEM((width, 4 * hid), BF16),
            pltpu.VMEM((2 * hid, width), BF16),
            pltpu.VMEM((zb, rows, 2 * wide), BF16),
            pltpu.SemaphoreType.DMA((width // fblk, 6)),
            pltpu.SemaphoreType.DMA((2 * zb * za,)),
        ],
        mib=24,
        flops=12 * product,
    )(got0, *(pltpu.with_memory_space_constraint(w, pltpu.HBM) for w in (w1, w3, w2, v1, v3, v2)))
    home = lax.all_to_all(ours.reshape(peers, CAP, 2 * wide), PEERS, 0, 0, tiled=True)
    home = home.reshape(zb, EXPERTS * yl * CAP, 2 * wide)

    got1 = lax.ppermute(got0, "c", swap)
    their_acts = lax.ppermute(their_acts, "c", swap)
    tall = pl.BlockSpec((fblk, hid), lambda t: (t, 0))
    flat = pl.BlockSpec((hid, fblk), lambda t: (0, t))
    grad_gate, grad_up, grad_down, done = call(
        weight_grad_kernel,
        "weight_grad",
        4,
        [((width, hid), BF16)] * 2 + [((hid, width), BF16), ((8, 128), F32)],
        grid=(width // fblk,),
        out_specs=[tall, tall, flat, pl.BlockSpec((8, 128), lambda t: (0, 0))],
        flops=6 * product,
        nbytes=6 * width * hid,
    )(got0, got1, acts, their_acts)

    (mixed,) = call(combine_kernel, "combine", 5, [((za, 2 * n_tok, fblk), BF16)])(
        high, low, hit, home, done
    )
    parts = lax.all_to_all(mixed, "za", 0, 0, tiled=True)
    total = jnp.sum(parts.astype(F32), axis=0)
    output, input_grad = total[:n_tok].astype(BF16), total[n_tok:].astype(BF16)
    return output, input_grad, grad_gate[None], grad_up[None], grad_down[None]


def solution(mesh):
    group = mesh.shape["exp"] // EXPERTS
    shape = (EXPERTS // 2, 2, group // 2, 2, mesh.shape["tp"] // 2, 2)
    fine = Mesh(mesh.devices.reshape(shape), EXP_AXES + TP_AXES)
    spec = (
        P(EXP_AXES, TP_AXES),
        P(EXP_AXES, TP_AXES),
        P(EXP_AXES, None),
        P(EXP_AXES, None),
        P(EXP_AXES, None, TP_AXES),
        P(EXP_AXES, None, TP_AXES),
        P(EXP_AXES, TP_AXES, None),
    )
    out = (spec[0], spec[1], spec[4], spec[5], spec[6])
    return jax.shard_map(per_device, mesh=fine, in_specs=spec, out_specs=out, check_vma=False)
```

```python
import functools
import math

import jax
import jax.numpy as jnp
from jax import lax
from jax.experimental import pallas as pl
from jax.experimental.pallas import tpu as pltpu
from jax.sharding import Mesh, PartitionSpec as P


EXPERTS = 8
CAP = 8

EXP_AXES = ("x", "yh", "yl", "c")
TP_AXES = ("za", "zb")
PEERS = ("zb", "x", "yh", "yl")
F32, BF16 = jnp.float32, jnp.bfloat16


def mm(a, b):
    return jnp.dot(a, b, preferred_element_type=F32)


def mm_nt(a, b):
    return lax.dot_general(a, b, (((1,), (1,)), ((), ())), preferred_element_type=F32)


def mm_tn(a, b):
    return lax.dot_general(a, b, (((0,), (0,)), ((), ())), preferred_element_type=F32)


def slot_hits(exp_ref, gate_ref, rows, group):
    n_tok = exp_ref.shape[1]
    r = lax.broadcasted_iota(jnp.int32, (rows, n_tok), 0)
    k, s = r // group, r % CAP
    first, second = exp_ref[0:1, :] == k, exp_ref[1:2, :] == k
    named = (first | second).astype(F32)
    before_of = lax.broadcasted_iota(jnp.int32, (n_tok, n_tok), 0) < lax.broadcasted_iota(
        jnp.int32, (n_tok, n_tok), 1
    )
    before = mm(named.astype(BF16), before_of.astype(F32).astype(BF16))
    hit = jnp.where(before == s.astype(F32), named, 0.0)
    gate = jnp.where(first, gate_ref[0:1, :], 0.0) + jnp.where(second, gate_ref[1:2, :], 0.0)
    return hit, hit * gate


def lane_shift(n_tok, by):
    row = lax.broadcasted_iota(jnp.int32, (n_tok, 2 * n_tok), 0)
    lane = lax.broadcasted_iota(jnp.int32, (n_tok, 2 * n_tok), 1)
    return (lane == row + by).astype(F32).astype(BF16)


def route_kernel(exp_ref, gate_ref, x_ref, g_ref, scale_ref, high_ref, low_ref, hit_ref, *, group):
    n_tok = exp_ref.shape[1]
    left, right = lane_shift(n_tok, 0), lane_shift(n_tok, n_tok)
    hit, weighted = slot_hits(exp_ref, gate_ref, EXPERTS * CAP, CAP)
    x_ref[...] = mm(hit.astype(BF16), left).astype(BF16)
    g_ref[...] = mm(hit.astype(BF16), right).astype(BF16)
    scale_ref[...] = jnp.broadcast_to(jnp.sum(weighted, axis=1, keepdims=True), scale_ref.shape)

    rows = EXPERTS * group
    hit, weighted = slot_hits(exp_ref, gate_ref, rows, group)
    high = weighted.astype(BF16)
    low = (weighted - high.astype(F32)).astype(BF16)
    same = (
        lax.broadcasted_iota(jnp.int32, (rows, rows), 0)
        == lax.broadcasted_iota(jnp.int32, (rows, rows), 1)
    )
    same = same.astype(F32).astype(BF16)
    for ref, table, side in ((high_ref, high, left), (low_ref, low, left), (hit_ref, hit, right)):
        ref[...] = mm_tn(mm(table.astype(BF16), side).astype(BF16), same).astype(BF16)


def dispatch_kernel(x_ref, g_ref, scale_ref, in_ref, out_ref):
    zb, _, yl, _, _ = out_ref.shape
    blocks, _, fblk = in_ref.shape
    for b in range(blocks):
        x = mm(x_ref[...], in_ref[b])
        g = mm(g_ref[...], in_ref[b]) * scale_ref[:, :1]
        for part, value in enumerate((x, g)):
            value = value.reshape(EXPERTS, CAP, fblk).astype(BF16)
            at = (part * blocks + b) * fblk
            for i in range(zb):
                for j in range(yl):
                    out_ref[i, :, j, :, at : at + fblk] = value


def mark_kernel(got, out_ref):
    out_ref[...] = got[0, :8, :128].astype(F32)


def rows_kernel(got, w1, w3, w2, v1, v3, v2, acts, their_acts, out_ref, up, down, total, in_sems, sems):
    pairs, _, wide = got.shape
    half, hid = wide // 2, w1.shape[1]
    steps = in_sems.shape[0]
    fblk = w1.shape[0] // steps
    loads = []
    for t in range(steps):
        span = slice(t * fblk, (t + 1) * fblk)
        block = [
            pltpu.make_async_copy(w.at[span], up.at[span, i * hid : (i + 1) * hid], in_sems.at[t, i])
            for i, w in enumerate((w1, v1, w3, v3))
        ]
        block += [
            pltpu.make_async_copy(
                w.at[:, span], down.at[i * hid : (i + 1) * hid, span], in_sems.at[t, 4 + i]
            )
            for i, w in enumerate((w2, v2))
        ]
        for load in block:
            load.start()
        loads.append(block)

    first = second = third = 0.0
    for t in range(steps):
        for load in loads[t]:
            load.wait()
        p, at = t % pairs, t // pairs * fblk
        span = slice(t * fblk, (t + 1) * fblk)
        x, g = got[p, :, at : at + fblk], got[p, :, half + at : half + at + fblk]
        first = first + mm(x, up[span, : 2 * hid])
        second = second + mm(x, up[span, 2 * hid :])
        third = third + mm_nt(g, down[:, span])
    sig = jax.nn.sigmoid(first)
    act = (first * sig * second).astype(BF16)
    d1 = (third * second * sig * (1.0 + first * (1.0 - sig))).astype(BF16)
    d3 = (third * first * sig).astype(BF16)
    for i, value in enumerate((act, d1, d3)):
        acts[i] = value[:, :hid]
        their_acts[i] = value[:, hid:]
    both = jnp.concatenate([d1, d3], axis=1)

    copies = []
    cut = fblk // 2
    for t in range(steps):
        p, at = t % pairs, t // pairs * fblk
        for i in range(2):
            span = slice(t * fblk + i * cut, t * fblk + (i + 1) * cut)
            here = at + i * cut
            total[p, :, here : here + cut] = mm(act, down[:, span]).astype(BF16)
            total[p, :, half + here : half + here + cut] = mm_nt(both, up[span, :]).astype(BF16)
        for base in (0, half):
            lanes = slice(base + at, base + at + fblk)
            copies.append(
                pltpu.make_async_copy(
                    total.at[p, :, lanes], out_ref.at[p, :, lanes], sems.at[len(copies)]
                )
            )
            copies[-1].start()
    for copy in copies:
        copy.wait()


def weight_grad_kernel(got0, got1, acts0, acts1, _, gg_ref, gu_ref, gd_ref, done_ref):
    t = pl.program_id(0)
    pairs, _, wide = got0.shape
    fblk = gg_ref.shape[0]
    p, b = lax.rem(t, pairs), lax.div(t, pairs)
    x_at = pl.ds(pl.multiple_of(b * fblk, fblk), fblk)
    g_at = pl.ds(pl.multiple_of(wide // 2 + b * fblk, fblk), fblk)
    x = jnp.concatenate([got0[p, :, x_at], got1[p, :, x_at]], axis=0)
    g = jnp.concatenate([got0[p, :, g_at], got1[p, :, g_at]], axis=0)
    act, d1, d3 = (jnp.concatenate([acts0[i], acts1[i]], axis=0) for i in range(3))
    gg_ref[...] = mm_tn(x, d1).astype(BF16)
    gu_ref[...] = mm_tn(x, d3).astype(BF16)
    gd_ref[...] = mm_tn(act, g).astype(BF16)
    done_ref[...] = jnp.zeros_like(done_ref)


def combine_kernel(high_ref, low_ref, hit_ref, home_ref, _, out_ref):
    pairs, _, wide = home_ref.shape
    blocks, _, fblk = out_ref.shape
    for b in range(blocks):
        out = 0.0
        for p in range(pairs):
            y = home_ref[p, :, b * fblk : (b + 1) * fblk]
            dx = home_ref[p, :, wide // 2 + b * fblk : wide // 2 + (b + 1) * fblk]
            out = out + mm(high_ref[...], y) + mm(low_ref[...], y) + mm(hit_ref[...], dx)
        out_ref[b] = out.astype(BF16)


VMEM = pl.BlockSpec(memory_space=pltpu.VMEM)
HBM = pl.BlockSpec(memory_space=pltpu.HBM)


def call(kernel, ins, outs, grid=(), out_specs=None, scratch=(), mib=8, flops=0, nbytes=0):
    out_specs = out_specs or [VMEM] * len(outs)
    return pl.pallas_call(
        kernel,
        grid=grid,
        in_specs=[VMEM] * ins if isinstance(ins, int) else ins,
        out_specs=out_specs,
        out_shape=[
            (pltpu.HBM if spec is HBM else jax.ShapeDtypeStruct)(shape, dtype)
            for (shape, dtype), spec in zip(outs, out_specs)
        ],
        scratch_shapes=list(scratch),
        compiler_params=pltpu.CompilerParams(vmem_limit_bytes=mib * 1024 * 1024),
        cost_estimate=pl.CostEstimate(flops=flops, bytes_accessed=nbytes, transcendentals=0),
    )


def per_device(tokens, cotangent, experts, gates, w_gate, w_up, w_down):
    za, zb, yl = (lax.axis_size(a) for a in ("za", "zb", "yl"))
    peers = math.prod(lax.axis_size(a) for a in PEERS)
    n_tok, fblk = tokens.shape
    w1, w3, w2 = w_gate[0], w_up[0], w_down[0]
    width, hid = w1.shape
    wide = za * fblk
    rows = peers // zb * CAP
    swap = [(0, 1), (1, 0)]
    v1, v3, v2 = (lax.ppermute(w, "c", swap) for w in (w1, w3, w2))

    both = jnp.concatenate([tokens, cotangent], axis=0)
    spread = jnp.broadcast_to(both[None], (za,) + both.shape)
    mine = lax.all_to_all(spread, "za", 0, 0, tiled=True)
    table = ((2 * n_tok, EXPERTS * yl * CAP), BF16)
    pick = ((EXPERTS * CAP, 2 * n_tok), BF16)
    pick_x, pick_g, scale, high, low, hit = call(
        functools.partial(route_kernel, group=yl * CAP),
        2,
        [pick, pick, ((EXPERTS * CAP, 128), F32)] + [table] * 3,
    )(experts.T, gates.T)

    (send,) = call(dispatch_kernel, 4, [((zb, EXPERTS, yl, CAP, 2 * wide), BF16)])(
        pick_x, pick_g, scale, mine
    )
    send = send.reshape(peers, CAP, 2 * wide)
    got0 = lax.all_to_all(send, PEERS, 0, 0, tiled=True).reshape(zb, rows, 2 * wide)

    (mark,) = call(mark_kernel, 1, [((8, 128), F32)])(got0)

    product = 2 * rows * width * hid
    acts, their_acts, ours = call(
        rows_kernel,
        [VMEM] + [HBM] * 6,
        [((3, rows, hid), BF16)] * 2 + [((zb, rows, 2 * wide), BF16)],
        out_specs=[VMEM, VMEM, HBM],
        scratch=[
            pltpu.VMEM((width, 4 * hid), BF16),
            pltpu.VMEM((2 * hid, width), BF16),
            pltpu.VMEM((zb, rows, 2 * wide), BF16),
            pltpu.SemaphoreType.DMA((width // fblk, 6)),
            pltpu.SemaphoreType.DMA((2 * zb * za,)),
        ],
        mib=24,
        flops=12 * product,
    )(got0, *(pltpu.with_memory_space_constraint(w, pltpu.HBM) for w in (w1, w3, w2, v1, v3, v2)))
    home = lax.all_to_all(ours.reshape(peers, CAP, 2 * wide), PEERS, 0, 0, tiled=True)
    home = home.reshape(zb, EXPERTS * yl * CAP, 2 * wide)

    got1 = lax.ppermute(got0, "c", swap)
    their_acts = lax.ppermute(their_acts, "c", swap)
    tall = pl.BlockSpec((fblk, hid), lambda t: (t, 0))
    flat = pl.BlockSpec((hid, fblk), lambda t: (0, t))
    grad_gate, grad_up, grad_down, done = call(
        weight_grad_kernel,
        5,
        [((width, hid), BF16)] * 2 + [((hid, width), BF16), ((8, 128), F32)],
        grid=(width // fblk,),
        out_specs=[tall, tall, flat, pl.BlockSpec((8, 128), lambda t: (0, 0))],
        flops=6 * product,
        nbytes=6 * width * hid,
    )(got0, got1, acts, their_acts, mark)

    (mixed,) = call(combine_kernel, 5, [((za, 2 * n_tok, fblk), BF16)])(high, low, hit, home, done)
    parts = lax.all_to_all(mixed, "za", 0, 0, tiled=True)
    total = jnp.sum(parts.astype(F32), axis=0)
    output, input_grad = total[:n_tok].astype(BF16), total[n_tok:].astype(BF16)
    return output, input_grad, grad_gate[None], grad_up[None], grad_down[None]


def solution(mesh):
    group = mesh.shape["exp"] // EXPERTS
    shape = (EXPERTS // 2, 2, group // 2, 2, mesh.shape["tp"] // 2, 2)
    fine = Mesh(mesh.devices.reshape(shape), EXP_AXES + TP_AXES)
    spec = (
        P(EXP_AXES, TP_AXES),
        P(EXP_AXES, TP_AXES),
        P(EXP_AXES, None),
        P(EXP_AXES, None),
        P(EXP_AXES, None, TP_AXES),
        P(EXP_AXES, None, TP_AXES),
        P(EXP_AXES, TP_AXES, None),
    )
    out = (spec[0], spec[1], spec[4], spec[5], spec[6])
    return jax.shard_map(per_device, mesh=fine, in_specs=spec, out_specs=out, check_vma=False)
```

```python
import functools
import math

import jax
import jax.numpy as jnp
from jax import lax
from jax.experimental import pallas as pl
from jax.experimental.pallas import tpu as pltpu
from jax.sharding import Mesh, PartitionSpec as P


EXPERTS = 8
CAP = 8

EXP_AXES = ("x", "yh", "yl", "c")
TP_AXES = ("za", "zb")
PEERS = ("zb", "x", "yh", "yl")
F32, BF16 = jnp.float32, jnp.bfloat16


def mm(a, b):
    return jnp.dot(a, b, preferred_element_type=F32)


def mm_nt(a, b):
    return lax.dot_general(a, b, (((1,), (1,)), ((), ())), preferred_element_type=F32)


def mm_tn(a, b):
    return lax.dot_general(a, b, (((0,), (0,)), ((), ())), preferred_element_type=F32)


def slot_hits(exp_ref, gate_ref, rows, group):
    n_tok = exp_ref.shape[1]
    r = lax.broadcasted_iota(jnp.int32, (rows, n_tok), 0)
    k, s = r // group, r % CAP
    first, second = exp_ref[0:1, :] == k, exp_ref[1:2, :] == k
    named = (first | second).astype(F32)
    before_of = lax.broadcasted_iota(jnp.int32, (n_tok, n_tok), 0) < lax.broadcasted_iota(
        jnp.int32, (n_tok, n_tok), 1
    )
    before = mm(named.astype(BF16), before_of.astype(F32).astype(BF16))
    hit = jnp.where(before == s.astype(F32), named, 0.0)
    gate = jnp.where(first, gate_ref[0:1, :], 0.0) + jnp.where(second, gate_ref[1:2, :], 0.0)
    return hit, hit * gate


def lane_shift(n_tok, by):
    row = lax.broadcasted_iota(jnp.int32, (n_tok, 2 * n_tok), 0)
    lane = lax.broadcasted_iota(jnp.int32, (n_tok, 2 * n_tok), 1)
    return (lane == row + by).astype(F32).astype(BF16)


def route_kernel(exp_ref, gate_ref, x_ref, g_ref, scale_ref, high_ref, low_ref, hit_ref, *, group):
    n_tok = exp_ref.shape[1]
    left, right = lane_shift(n_tok, 0), lane_shift(n_tok, n_tok)
    hit, weighted = slot_hits(exp_ref, gate_ref, EXPERTS * CAP, CAP)
    x_ref[...] = mm(hit.astype(BF16), left).astype(BF16)
    g_ref[...] = mm(hit.astype(BF16), right).astype(BF16)
    scale_ref[...] = jnp.broadcast_to(jnp.sum(weighted, axis=1, keepdims=True), scale_ref.shape)

    rows = EXPERTS * group
    hit, weighted = slot_hits(exp_ref, gate_ref, rows, group)
    high = weighted.astype(BF16)
    low = (weighted - high.astype(F32)).astype(BF16)
    same = (
        lax.broadcasted_iota(jnp.int32, (rows, rows), 0)
        == lax.broadcasted_iota(jnp.int32, (rows, rows), 1)
    )
    same = same.astype(F32).astype(BF16)
    for ref, table, side in ((high_ref, high, left), (low_ref, low, left), (hit_ref, hit, right)):
        ref[...] = mm_tn(mm(table.astype(BF16), side).astype(BF16), same).astype(BF16)


def dispatch_kernel(x_ref, g_ref, scale_ref, in_ref, out_ref):
    zb, _, yl, _, _ = out_ref.shape
    blocks, _, fblk = in_ref.shape
    for b in range(blocks):
        x = mm(x_ref[...], in_ref[b])
        g = mm(g_ref[...], in_ref[b]) * scale_ref[:, :1]
        for part, value in enumerate((x, g)):
            value = value.reshape(EXPERTS, CAP, fblk).astype(BF16)
            at = (part * blocks + b) * fblk
            for i in range(zb):
                for j in range(yl):
                    out_ref[i, :, j, :, at : at + fblk] = value


def mark_kernel(got, out_ref):
    out_ref[...] = got[0, :8, :128].astype(F32)


def rows_kernel(got, w1, w3, w2, v1, v3, v2, acts, their_acts, out_ref, up, down, total, in_sems, sems):
    pairs, _, wide = got.shape
    half, hid = wide // 2, w1.shape[1]
    steps = in_sems.shape[0]
    fblk = w1.shape[0] // steps
    loads = []
    for t in range(steps):
        span = slice(t * fblk, (t + 1) * fblk)
        block = [
            pltpu.make_async_copy(w.at[span], up.at[span, i * hid : (i + 1) * hid], in_sems.at[t, i])
            for i, w in enumerate((w1, v1, w3, v3))
        ]
        block += [
            pltpu.make_async_copy(
                w.at[:, span], down.at[i * hid : (i + 1) * hid, span], in_sems.at[t, 4 + i]
            )
            for i, w in enumerate((w2, v2))
        ]
        for load in block:
            load.start()
        loads.append(block)

    first = second = third = 0.0
    for t in range(steps):
        for load in loads[t]:
            load.wait()
        p, at = t % pairs, t // pairs * fblk
        span = slice(t * fblk, (t + 1) * fblk)
        x, g = got[p, :, at : at + fblk], got[p, :, half + at : half + at + fblk]
        first = first + mm(x, up[span, : 2 * hid])
        second = second + mm(x, up[span, 2 * hid :])
        third = third + mm_nt(g, down[:, span])
    sig = jax.nn.sigmoid(first)
    act = (first * sig * second).astype(BF16)
    d1 = (third * second * sig * (1.0 + first * (1.0 - sig))).astype(BF16)
    d3 = (third * first * sig).astype(BF16)
    for i, value in enumerate((act, d1, d3)):
        acts[i] = value[:, :hid]
        their_acts[i] = value[:, hid:]
    both = jnp.concatenate([d1, d3], axis=1)

    copies = []
    cut = fblk // 2
    for t in range(steps):
        p, at = t % pairs, t // pairs * fblk
        for i in range(2):
            span = slice(t * fblk + i * cut, t * fblk + (i + 1) * cut)
            here = at + i * cut
            total[p, :, here : here + cut] = mm(act, down[:, span]).astype(BF16)
            total[p, :, half + here : half + here + cut] = mm_nt(both, up[span, :]).astype(BF16)
        for base in (0, half):
            lanes = slice(base + at, base + at + fblk)
            copies.append(
                pltpu.make_async_copy(
                    total.at[p, :, lanes], out_ref.at[p, :, lanes], sems.at[len(copies)]
                )
            )
            copies[-1].start()
    for copy in copies:
        copy.wait()


def weight_grad_kernel(got0, got1, acts0, acts1, _, gg_ref, gu_ref, gd_ref, done_ref):
    t = pl.program_id(0)
    pairs, _, wide = got0.shape
    fblk = gg_ref.shape[0]
    p, b = lax.rem(t, pairs), lax.div(t, pairs)
    x_at = pl.ds(pl.multiple_of(b * fblk, fblk), fblk)
    g_at = pl.ds(pl.multiple_of(wide // 2 + b * fblk, fblk), fblk)
    x = jnp.concatenate([got0[p, :, x_at], got1[p, :, x_at]], axis=0)
    g = jnp.concatenate([got0[p, :, g_at], got1[p, :, g_at]], axis=0)
    act, d1, d3 = (jnp.concatenate([acts0[i], acts1[i]], axis=0) for i in range(3))
    gg_ref[...] = mm_tn(x, d1).astype(BF16)
    gu_ref[...] = mm_tn(x, d3).astype(BF16)
    gd_ref[...] = mm_tn(act, g).astype(BF16)
    done_ref[...] = jnp.zeros_like(done_ref)


def combine_kernel(high_ref, low_ref, hit_ref, y_ref, dx_ref, _, out_ref):
    out = 0.0
    for p in range(y_ref.shape[0]):
        out = out + mm(high_ref[...], y_ref[p]) + mm(low_ref[...], y_ref[p])
        out = out + mm(hit_ref[...], dx_ref[p])
    out_ref[0] = out.astype(BF16)


VMEM = pl.BlockSpec(memory_space=pltpu.VMEM)
HBM = pl.BlockSpec(memory_space=pltpu.HBM)


def call(kernel, ins, outs, grid=(), out_specs=None, scratch=(), mib=8, flops=0, nbytes=0):
    out_specs = out_specs or [VMEM] * len(outs)
    return pl.pallas_call(
        kernel,
        grid=grid,
        in_specs=[VMEM] * ins if isinstance(ins, int) else ins,
        out_specs=out_specs,
        out_shape=[
            (pltpu.HBM if spec is HBM else jax.ShapeDtypeStruct)(shape, dtype)
            for (shape, dtype), spec in zip(outs, out_specs)
        ],
        scratch_shapes=list(scratch),
        compiler_params=pltpu.CompilerParams(vmem_limit_bytes=mib * 1024 * 1024),
        cost_estimate=pl.CostEstimate(flops=flops, bytes_accessed=nbytes, transcendentals=0),
    )


def per_device(tokens, cotangent, experts, gates, w_gate, w_up, w_down):
    za, zb, yl = (lax.axis_size(a) for a in ("za", "zb", "yl"))
    peers = math.prod(lax.axis_size(a) for a in PEERS)
    n_tok, fblk = tokens.shape
    w1, w3, w2 = w_gate[0], w_up[0], w_down[0]
    width, hid = w1.shape
    wide = za * fblk
    rows = peers // zb * CAP
    swap = [(0, 1), (1, 0)]
    v1, v3, v2 = (lax.ppermute(w, "c", swap) for w in (w1, w3, w2))

    both = jnp.concatenate([tokens, cotangent], axis=0)
    spread = jnp.broadcast_to(both[None], (za,) + both.shape)
    mine = lax.all_to_all(spread, "za", 0, 0, tiled=True)
    table = ((2 * n_tok, EXPERTS * yl * CAP), BF16)
    pick = ((EXPERTS * CAP, 2 * n_tok), BF16)
    pick_x, pick_g, scale, high, low, hit = call(
        functools.partial(route_kernel, group=yl * CAP),
        2,
        [pick, pick, ((EXPERTS * CAP, 128), F32)] + [table] * 3,
    )(experts.T, gates.T)

    (send,) = call(dispatch_kernel, 4, [((zb, EXPERTS, yl, CAP, 2 * wide), BF16)])(
        pick_x, pick_g, scale, mine
    )
    send = send.reshape(peers, CAP, 2 * wide)
    got0 = lax.all_to_all(send, PEERS, 0, 0, tiled=True).reshape(zb, rows, 2 * wide)

    (mark,) = call(mark_kernel, 1, [((8, 128), F32)])(got0)

    product = 2 * rows * width * hid
    acts, their_acts, ours = call(
        rows_kernel,
        [VMEM] + [HBM] * 6,
        [((3, rows, hid), BF16)] * 2 + [((zb, rows, 2 * wide), BF16)],
        out_specs=[VMEM, VMEM, HBM],
        scratch=[
            pltpu.VMEM((width, 4 * hid), BF16),
            pltpu.VMEM((2 * hid, width), BF16),
            pltpu.VMEM((zb, rows, 2 * wide), BF16),
            pltpu.SemaphoreType.DMA((width // fblk, 6)),
            pltpu.SemaphoreType.DMA((2 * zb * za,)),
        ],
        mib=24,
        flops=12 * product,
    )(got0, *(pltpu.with_memory_space_constraint(w, pltpu.HBM) for w in (w1, w3, w2, v1, v3, v2)))
    home = lax.all_to_all(ours.reshape(peers, CAP, 2 * wide), PEERS, 0, 0, tiled=True)
    home = home.reshape(zb, EXPERTS * yl * CAP, 2 * wide)

    got1 = lax.ppermute(got0, "c", swap)
    their_acts = lax.ppermute(their_acts, "c", swap)
    tall = pl.BlockSpec((fblk, hid), lambda t: (t, 0))
    flat = pl.BlockSpec((hid, fblk), lambda t: (0, t))
    grad_gate, grad_up, grad_down, done = call(
        weight_grad_kernel,
        5,
        [((width, hid), BF16)] * 2 + [((hid, width), BF16), ((8, 128), F32)],
        grid=(width // fblk,),
        out_specs=[tall, tall, flat, pl.BlockSpec((8, 128), lambda t: (0, 0))],
        flops=6 * product,
        nbytes=6 * width * hid,
    )(got0, got1, acts, their_acts, mark)

    home = pltpu.with_memory_space_constraint(home, pltpu.HBM)
    block = (zb, EXPERTS * yl * CAP, fblk)
    (mixed,) = call(
        combine_kernel,
        [VMEM] * 3
        + [pl.BlockSpec(block, lambda b: (0, 0, b)), pl.BlockSpec(block, lambda b: (0, 0, za + b)), VMEM],
        [((za, 2 * n_tok, fblk), BF16)],
        grid=(za,),
        out_specs=[pl.BlockSpec((1, 2 * n_tok, fblk), lambda b: (b, 0, 0))],
    )(high, low, hit, home, home, done)
    parts = lax.all_to_all(mixed, "za", 0, 0, tiled=True)
    total = jnp.sum(parts.astype(F32), axis=0)
    output, input_grad = total[:n_tok].astype(BF16), total[n_tok:].astype(BF16)
    return output, input_grad, grad_gate[None], grad_up[None], grad_down[None]


def solution(mesh):
    group = mesh.shape["exp"] // EXPERTS
    shape = (EXPERTS // 2, 2, group // 2, 2, mesh.shape["tp"] // 2, 2)
    fine = Mesh(mesh.devices.reshape(shape), EXP_AXES + TP_AXES)
    spec = (
        P(EXP_AXES, TP_AXES),
        P(EXP_AXES, TP_AXES),
        P(EXP_AXES, None),
        P(EXP_AXES, None),
        P(EXP_AXES, None, TP_AXES),
        P(EXP_AXES, None, TP_AXES),
        P(EXP_AXES, TP_AXES, None),
    )
    out = (spec[0], spec[1], spec[4], spec[5], spec[6])
    return jax.shard_map(per_device, mesh=fine, in_specs=spec, out_specs=out, check_vma=False)
```
